32 devices in a mesh: tgt: 8 (over z, y), src: 4 (over x, core).
Axes of the slice: x: 2, y: 2, z: 4, core: 2. Of those that a mesh axis runs over, the one named last changes fastest.
Arguments:
- lattice: int32 [2, 1024], P(None, ('tgt', 'src')), may hold values from 0 to 63, as said below
- material: int32 [1024], P(('tgt', 'src')), may hold values from 0 to 15
- polarizability: float32 [4, 16, 4], replicated, may hold values from -1.2 to 1.2
- wavenumber: float32 [4], replicated, may hold values from 2 to 3.5
- dipoles: bfloat16 [4, 2, 6, 4, 1024], P(None, None, None, None, ('tgt', 'src')), may hold values from -6 to 6
- adjoint_in: bfloat16 [4, 2, 6, 4, 1024], P(None, None, None, None, ('tgt', 'src')), may hold values from -6 to 6
Outputs:
- forward_out: float32 [4, 2, 6, 4, 1024], P(None, None, None, None, ('tgt', 'src'))
- adjoint_out: float32 [4, 2, 6, 4, 1024], P(None, None, None, None, ('tgt', 'src'))
The draws below stay inside these ranges and needn't reach their ends.
Inputs may be any that keep to these rules, and one draw needn't show every extreme that they name: Atoms are numbered tile by tile, the second tile index fastest; a tile spans 2 x 16 lattice sites, and its 32 atoms occupy each of its sites exactly once, in any order. The first index runs from 0 to 15, the second from 0 to 63.
All inputs are finite; a program needn't handle non-finite values.
Results may differ from the reference program's by a relative error of at most 0.0039.
Values may be sent and summed in bfloat16 or wider, within the bound.
No kernel may reach another device: no remote copies, remote signals or barrier semaphores. Data moves between devices by JAX's collectives and lax.ppermute only.
A program may use at most 64 MiB of HBM per device.

```python
import math
import jax
import jax.numpy as jnp
from jax import lax

WAVES = 4
EXCITE = 4
TYPES = 16
TILE_Y = 16
TILE_X = 2
ATOMS = 32
LATTICE_X = 16
LATTICE_Y = 64
ATOMS_ALL = 1024
N_TGT = 8
N_SRC = 4


def draw_lattice(key, part):
    columns = LATTICE_Y // TILE_Y
    blocks = LATTICE_X // TILE_X * columns
    subkeys = jax.random.split(jax.random.fold_in(key, 11), blocks)
    placed = jax.vmap(lambda subkey: jax.random.permutation(subkey, ATOMS))(subkeys).astype(jnp.int32)
    block_id = jnp.arange(blocks, dtype=jnp.int32)[:, None]
    first = block_id // columns * TILE_X + placed // TILE_Y
    second = block_id % columns * TILE_Y + placed % TILE_Y
    return jnp.stack([first.reshape(-1), second.reshape(-1)]).astype(jnp.int32)


def with_ends(values, own_key, smallest, top_value):
    longest = values.shape.index(max(values.shape))
    spots = []
    for shift in (0, 1):
        where = [jax.random.randint(jax.random.fold_in(own_key, axis), (), 0, length) for axis, length in enumerate(values.shape)]
        where[longest] = (where[longest] + shift) % values.shape[longest]
        spots.append(tuple(where))
    return values.at[spots[0]].set(smallest).at[spots[1]].set(top_value)


def block_scale(own_key, extent, cuts, least, high):
    factor_of = 1.0
    for dim, shards_of in cuts:
        steps = jax.random.uniform(jax.random.fold_in(jax.random.fold_in(own_key, 6), dim), (shards_of,), jnp.float32, least / len(cuts), high / len(cuts))
        factor_of = factor_of * jnp.repeat(jnp.exp(steps), extent[dim] // shards_of).reshape((-1,) + (1,) * (len(extent) - 1 - dim))
    return factor_of


def bell_draw(stream_key, shape, spread, most, cuts=(), kind=jnp.bfloat16):
    values = jax.random.normal(stream_key, shape, jnp.float32) * spread
    if len(cuts) > 0:
        values = block_scale(stream_key, shape, cuts, -0.22, 0.18) * values
    return jnp.clip(values, min=-most, max=most).astype(kind)


def setup_inputs(seed: int = 0) -> dict:
    streams_of = jax.random.split(jax.random.key(seed), 7)
    lattice = draw_lattice(jax.random.fold_in(streams_of[6], 71), 0)
    material = with_ends(jax.random.randint(streams_of[1], (ATOMS_ALL,), 0, TYPES), jax.random.fold_in(streams_of[1], 1), 0, TYPES - 1).astype(jnp.int32)
    polarizability = jnp.clip(jax.random.uniform(streams_of[2], (4, TYPES, WAVES), jnp.float32, -1.2, 1.2), -1.2, 1.2)
    wavenumber = jnp.clip(jnp.exp(jax.random.uniform(streams_of[3], (WAVES,), jnp.float32, math.log(2.0), math.log(3.5))), 2.0, 3.5)
    dipoles = bell_draw(streams_of[4], (WAVES, 2, 6, EXCITE, ATOMS_ALL), 1.0, 6.0, ((4, 32),))
    adjoint_in = bell_draw(streams_of[5], (WAVES, 2, 6, EXCITE, ATOMS_ALL), 1.0, 6.0, ((4, 32),))
    return dict(lattice=lattice, material=material, polarizability=polarizability, wavenumber=wavenumber, dipoles=dipoles, adjoint_in=adjoint_in)


COUPLINGS = ((0, 1, 0, 1.0), (0, 3, 1, 1.0), (0, 5, 5, 1.0), (1, 3, 0, 1.0), (1, 2, 1, 1.0), (1, 4, 5, -1.0), (2, 0, 2, 1.0), (2, 4, 4, 1.0), (2, 5, 3, -1.0), (3, 1, 3, 1.0), (3, 3, 4, 1.0), (3, 5, 2, -1.0), (4, 3, 3, 1.0), (4, 2, 4, 1.0), (4, 4, 2, 1.0), (5, 0, 5, 1.0), (5, 4, 1, -1.0), (5, 5, 0, 1.0))
KERNEL_SOURCES = ((0, (2, 5)), (1, (0, 3)), (2, (1, 4)), (3, (0, 1, 3, 4)), (4, (1, 2, 4, 5)), (5, (0, 2, 3, 5)))

def atom_polarizability(material, polarizability):
    kinds = jnp.arange(polarizability.shape[1], dtype=jnp.int32)
    onehot = (kinds[:, None] == material[None, :]).astype(jnp.float32)
    table = jnp.einsum('kyw,yn->kwn', polarizability, onehot, precision=lax.Precision.HIGHEST)
    alpha_re = jnp.stack([table[0]] * 3 + [table[2]] * 3, axis=1)[:, :, None, :]
    alpha_im = jnp.stack([table[1]] * 3 + [table[3]] * 3, axis=1)[:, :, None, :]
    return (alpha_re, alpha_im)

def pack_sources(dipoles, adjoint_in, alpha):
    alpha_re, alpha_im = alpha
    vector = adjoint_in.astype(jnp.float32)
    scaled_re = alpha_re * vector[:, 0] + alpha_im * vector[:, 1]
    scaled_im = alpha_re * vector[:, 1] - alpha_im * vector[:, 0]
    scaled = jnp.stack([scaled_re, scaled_im], axis=1).astype(jnp.bfloat16)
    return jnp.stack([dipoles, scaled], axis=1)

def green_kernels(geometry, wave):
    present, radius, unit_x, unit_y = geometry
    phase = wave * radius
    inverse = 1.0 / phase
    weight = present * inverse
    green_re = jnp.cos(phase) * weight
    green_im = jnp.sin(phase) * weight
    inv_sq = inverse * inverse
    near_re = green_re * (1.0 - inv_sq) - green_im * inverse
    near_im = green_im * (1.0 - inv_sq) + green_re * inverse
    long_re = green_re * (3.0 * inv_sq - 1.0) + 3.0 * green_im * inverse
    long_im = green_im * (3.0 * inv_sq - 1.0) - 3.0 * green_re * inverse
    cross_re = green_re - green_im * inverse
    cross_im = green_im + green_re * inverse
    xx_unit = unit_x * unit_x
    yy_unit = unit_y * unit_y
    xy_unit = unit_x * unit_y
    return jnp.stack([jnp.stack([near_re, near_im]), jnp.stack([near_re + long_re * xx_unit, near_im + long_im * xx_unit]), jnp.stack([near_re + long_re * yy_unit, near_im + long_im * yy_unit]), jnp.stack([long_re * xy_unit, long_im * xy_unit]), jnp.stack([cross_re * unit_x, cross_im * unit_x]), jnp.stack([cross_re * unit_y, cross_im * unit_y])]).astype(jnp.bfloat16)

def kernel_products(values, kernel_pair, kernel_index, components):
    sources = values.shape[-1]
    excite = values.shape[-2]
    targets = kernel_pair.shape[-1]
    count = len(components)
    picked = jnp.stack([values[:, :, comp] for comp in components]).reshape(-1, sources)
    with_re = jnp.dot(picked, kernel_pair[0], preferred_element_type=jnp.float32).reshape(count, 2, 2, excite, targets)
    with_im = jnp.dot(picked, kernel_pair[1], preferred_element_type=jnp.float32).reshape(count, 2, 2, excite, targets)
    fwd_re = with_re[:, 0, 0] - with_im[:, 0, 1]
    fwd_im = with_re[:, 0, 1] + with_im[:, 0, 0]
    adj_re = with_re[:, 1, 0] + with_im[:, 1, 1]
    adj_im = with_re[:, 1, 1] - with_im[:, 1, 0]
    if kernel_index >= 4:
        adj_re = -adj_re
        adj_im = -adj_im
    return jnp.stack([fwd_re, fwd_im, adj_re, adj_im], axis=1)

def column_fields(target_sites, source_sites, values, wavenumber, period):
    delta_x = target_sites[0][None, :] - source_sites[0][:, None]
    delta_y = target_sites[1][None, :] - source_sites[1][:, None]
    delta_y = jnp.where(2 * delta_y > period, delta_y - period, jnp.where(2 * delta_y < -period, delta_y + period, delta_y))
    delta_x = delta_x.astype(jnp.float32)
    delta_y = delta_y.astype(jnp.float32)
    radius_sq = delta_x * delta_x + delta_y * delta_y
    present = radius_sq > 0.5
    radius = jnp.sqrt(jnp.where(present, radius_sq, 1.0))
    geometry = (present.astype(jnp.float32), radius, delta_x / radius, delta_y / radius)
    targets = target_sites.shape[1]
    per_wave = []
    for wave_index in range(values.shape[0]):
        kernels = green_kernels(geometry, wavenumber[wave_index])
        products = {}
        for kernel_index, components in KERNEL_SOURCES:
            products[kernel_index] = kernel_products(values[wave_index], kernels[kernel_index], kernel_index, components)
        outputs = []
        for target_comp in range(6):
            summed = None
            for out_comp, kernel_index, source_comp, sign in COUPLINGS:
                if out_comp == target_comp:
                    place = dict(KERNEL_SOURCES)[kernel_index].index(source_comp)
                    term = sign * products[kernel_index][place]
                    summed = term if summed is None else summed + term
            outputs.append(summed)
        per_wave.append(jnp.stack(outputs, axis=1))
    return jnp.stack(per_wave).reshape(-1, targets)

def finish_outputs(fields, dipoles, adjoint_in, alpha):
    alpha_re, alpha_im = alpha
    shaped = fields.reshape((dipoles.shape[0], 2) + dipoles.shape[1:])
    forward_field = shaped[:, 0]
    adjoint_field = shaped[:, 1]
    source = dipoles.astype(jnp.float32)
    out_re = source[:, 0] - (alpha_re * forward_field[:, 0] - alpha_im * forward_field[:, 1])
    out_im = source[:, 1] - (alpha_re * forward_field[:, 1] + alpha_im * forward_field[:, 0])
    forward_out = jnp.stack([out_re, out_im], axis=1)
    adjoint_out = adjoint_in.astype(jnp.float32) - adjoint_field
    return (forward_out, adjoint_out)

def reference(lattice, material, polarizability, wavenumber, dipoles, adjoint_in):
    alpha = atom_polarizability(material, polarizability)
    values = pack_sources(dipoles, adjoint_in, alpha)
    blocks = values.reshape(values.shape[:-1] + (N_TGT, N_SRC, ATOMS))
    sites = lattice.reshape(2, N_TGT, N_SRC, ATOMS)
    period = N_SRC * TILE_Y
    field_rows = 24 * WAVES * EXCITE

    def one_column(column):
        target_sites = sites[:, :, column, :].reshape(2, N_TGT * ATOMS)

        def absorb(step, total):
            offset = step // N_TGT
            band = step % N_TGT
            source_column = (column + offset + N_SRC - 1) % N_SRC
            source_sites = sites[:, band, source_column, :]
            source_values = blocks[:, :, :, :, :, band, source_column, :]
            return total + column_fields(target_sites, source_sites, source_values, wavenumber, period)
        start_total = jnp.zeros((field_rows, N_TGT * ATOMS), jnp.float32)
        return lax.fori_loop(0, 3 * N_TGT, absorb, start_total)
    per_column = lax.map(one_column, jnp.arange(N_SRC, dtype=jnp.int32))
    per_column = per_column.reshape(N_SRC, field_rows, N_TGT, ATOMS)
    fields = jnp.transpose(per_column, (1, 2, 0, 3)).reshape(field_rows, ATOMS_ALL)
    return finish_outputs(fields, dipoles, adjoint_in, alpha)
```

```python
import functools

import jax
import jax.numpy as jnp
from jax import lax
from jax.experimental import pallas as pl
from jax.experimental.pallas import tpu as pltpu
from jax.sharding import PartitionSpec as P

TILE_Y = 16
TILE_X = 2
ATOMS = TILE_X * TILE_Y
AXES = ("tgt", "src")
BANDS = 2

SETS = ((0, 1, 5), (3, 4, 2))
PLACES = (((0, 0),), ((1, 1),), ((2, 2),), ((1, 0), (0, 1)), ((2, 0), (0, 2)), ((2, 1), (1, 2)))


def z_partner(z, shift, count):
    return z ^ shift if count & (count - 1) == 0 else (z + shift) % count


def column_partner(s, slot, count):
    if slot == 0:
        return s
    if count % 2:
        return (s + (1 if slot == 1 else -1)) % count
    step = 1 if (s % 2 == 0) == (slot == 1) else -1
    return (s + step) % count


def pairs(n_tgt, n_src, shift, flip, slot):
    depth = n_tgt // BANDS
    out = []
    for t in range(n_tgt):
        z, y = divmod(t, BANDS)
        for s in range(n_src):
            to_t = z_partner(z, shift, depth) * BANDS + (y + flip) % BANDS
            out.append((t * n_src + s, to_t * n_src + column_partner(s, slot, n_src)))
    return out


def site_of(lattice):
    return (lattice[0:1] % TILE_X) * TILE_Y + lattice[1:2] % TILE_Y


def pack_kernel(lattice_ref, material_ref, pol_ref, dip_ref, adj_ref, payload_ref, alpha_ref):
    waves, _, _, excite, atoms = dip_ref.shape
    types = pol_ref.shape[2]
    kinds = lax.broadcasted_iota(jnp.int32, (types, atoms), 0)
    onehot = jnp.where(kinds == material_ref[...], 1.0, 0.0).astype(jnp.float32)
    alpha = []
    for kind in range(4):
        value = jnp.dot(
            pol_ref[kind], onehot, precision=lax.Precision.HIGHEST, preferred_element_type=jnp.float32
        )
        alpha_ref[kind] = value
        alpha.append(value)
    rows = []
    for w in range(waves):
        fwd = {}
        adj = {}
        for comp in range(6):
            base = 0 if comp < 3 else 2
            a_re = alpha[base][w : w + 1]
            a_im = alpha[base + 1][w : w + 1]
            v_re = adj_ref[w, 0, comp].astype(jnp.float32)
            v_im = adj_ref[w, 1, comp].astype(jnp.float32)
            fwd[comp] = (dip_ref[w, 0, comp].astype(jnp.float32), dip_ref[w, 1, comp].astype(jnp.float32))
            adj[comp] = (a_re * v_re + a_im * v_im, a_re * v_im - a_im * v_re)
        for c in range(3):
            first, second = SETS[0][c], SETS[1][c]
            for ri in range(2):
                f1 = fwd[first][ri]
                f2 = fwd[second][ri] if c < 2 else -fwd[second][ri]
                a1 = adj[first][ri]
                a2 = adj[second][ri]
                if ri == 1:
                    a1, a2 = -a1, -a2
                if c == 2:
                    a1 = -a1
                rows += [f1, f2, a1, a2]
    table = jnp.concatenate(rows, axis=0).astype(jnp.bfloat16)
    sites = lax.broadcasted_iota(jnp.int32, (atoms, atoms), 0)
    place = jnp.where(sites == site_of(lattice_ref[...]), 1.0, 0.0).astype(jnp.bfloat16)
    payload_ref[...] = lax.dot_general(
        place, table, (((1,), (1,)), ((), ())), preferred_element_type=jnp.float32
    ).astype(jnp.bfloat16)


def sin_cos(x):
    turns = jnp.floor(x * 0.6366197723675814 + 0.5)
    rest = ((x - turns * 1.5703125) - turns * 4.837512969970703125e-4) - turns * 7.54978995489188216e-8
    sq = rest * rest
    sin = rest + rest * sq * (-1.6666654611e-1 + sq * (8.3321608736e-3 - sq * 1.9515295891e-4))
    cos = 1.0 - 0.5 * sq + sq * sq * (4.166664568298827e-2 + sq * (-1.388731625493765e-3 + sq * 2.443315711809948e-5))
    quarter = turns.astype(jnp.int32)
    odd = (quarter & 1) == 1
    sin, cos = jnp.where(odd, cos, sin), jnp.where(odd, sin, cos)
    sin = jnp.where((quarter & 2) == 2, -sin, sin)
    cos = jnp.where(((quarter + 1) & 2) == 2, -cos, cos)
    return sin, cos


def green_kernel(wave_ref, out_ref, *, n_tgt, n_src):
    waves, _, double, targets = out_ref.shape
    sources = double // 2
    depth = n_tgt // BANDS
    band = lax.axis_index("tgt")
    column = lax.axis_index("src")
    z, y = band // BANDS, band % BANDS
    period = n_src * TILE_Y
    if n_src % 2:
        step = 1
    else:
        step = 1 - 2 * (column % 2)
    lane = lax.broadcasted_iota(jnp.int32, (1, targets), 1)
    slot = lane // (BANDS * ATOMS)
    offset = jnp.where(slot == 0, 0, jnp.where(slot == 1, step, -step))
    to_band = z * BANDS + (y + lane // ATOMS) % BANDS
    to_x = to_band * TILE_X + lane % ATOMS // TILE_Y
    to_y = offset * TILE_Y + lane % TILE_Y
    for k in range(depth):
        from_band = z_partner(z, k, depth) * BANDS + y
        row = lax.broadcasted_iota(jnp.int32, (ATOMS, 1), 0)
        dx = to_x - (from_band * TILE_X + row // TILE_Y)
        dy = to_y - row % TILE_Y
        dy = jnp.where(2 * dy > period, dy - period, jnp.where(2 * dy < -period, dy + period, dy))
        dx = dx.astype(jnp.float32)
        dy = dy.astype(jnp.float32)
        square = dx * dx + dy * dy
        inverse = jnp.where(square > 0.5, lax.rsqrt(jnp.maximum(square, 1.0)), 0.0)
        radius = square * inverse
        ux = dx * inverse
        uy = dy * inverse
        xx, yy, xy = ux * ux, uy * uy, ux * uy
        ux = -ux
        for w in range(waves):
            wave = wave_ref[w]
            sin, cos = sin_cos(wave * radius)
            inv = inverse * (1.0 / wave)
            g_re = cos * inv
            g_im = sin * inv
            h_re = g_re * inv
            h_im = g_im * inv
            e_re = h_re * inv + h_im
            e_im = h_im * inv - h_re
            near = (g_re - e_re, g_im - e_im)
            far = (3.0 * e_re - g_re, 3.0 * e_im - g_im)
            cross = (g_re - h_im, g_im + h_re)
            for part in range(2):
                there = pl.ds(part * sources + k * ATOMS, ATOMS)
                n, f, c = near[part], far[part], cross[part]
                out_ref[w, 0, there] = (n + f * xx).astype(jnp.bfloat16)
                out_ref[w, 1, there] = (n + f * yy).astype(jnp.bfloat16)
                out_ref[w, 2, there] = n.astype(jnp.bfloat16)
                out_ref[w, 3, there] = (f * xy).astype(jnp.bfloat16)
                out_ref[w, 4, there] = (c * uy).astype(jnp.bfloat16)
                out_ref[w, 5, there] = (c * ux).astype(jnp.bfloat16)


def field_kernel(*refs):
    *tile_refs, kernels_ref, own_ref, sent_ref = refs
    waves = kernels_ref.shape[0]
    gathered = jnp.concatenate([ref[...].astype(jnp.float32) for ref in tile_refs], axis=0)
    rows = gathered.T.astype(jnp.bfloat16)
    half = rows.shape[0] // (waves * 6)
    fields = []
    for w in range(waves):
        left = []
        for c in range(3):
            base = (w * 3 + c) * 2 * half
            re, im = rows[base : base + half], rows[base + half : base + 2 * half]
            left.append(
                jnp.concatenate(
                    [jnp.concatenate([re, -im], axis=1), jnp.concatenate([im, re], axis=1)], axis=0
                )
            )
        total = [None] * 3
        for index, places in enumerate(PLACES):
            stacked = jnp.concatenate([left[c_in] for c_in, _ in places], axis=0)
            product = jnp.dot(stacked, kernels_ref[w, index], preferred_element_type=jnp.float32)
            for number, (_, c_out) in enumerate(places):
                piece = product[number * 2 * half : (number + 1) * 2 * half]
                total[c_out] = piece if total[c_out] is None else total[c_out] + piece
        fields += total
    turned = jnp.concatenate(fields, axis=0).T
    own_ref[...] = turned[:ATOMS]
    for index in range(sent_ref.shape[0]):
        sent_ref[index] = turned[(index + 1) * ATOMS : (index + 2) * ATOMS].astype(jnp.bfloat16)


def finish_kernel(*refs):
    lattice_ref, alpha_ref, dip_ref, adj_ref, own_ref, *rest = refs
    *got_refs, fwd_ref, out_ref = rest
    waves, _, _, excite, atoms = dip_ref.shape
    field = own_ref[...]
    for ref in got_refs:
        field = field + ref[...].astype(jnp.float32)
    high = field.astype(jnp.bfloat16)
    low = (field - high.astype(jnp.float32)).astype(jnp.bfloat16)
    sites = lax.broadcasted_iota(jnp.int32, (atoms, atoms), 0)
    place = jnp.where(sites == site_of(lattice_ref[...]), 1.0, 0.0).astype(jnp.bfloat16)
    rows = lax.dot_general(
        jnp.concatenate([high, low], axis=0),
        jnp.concatenate([place, place], axis=0),
        (((0,), (0,)), ((), ())),
        preferred_element_type=jnp.float32,
    )
    for w in range(waves):
        for c in range(3):
            base = (w * 3 + c) * 8 * excite
            pick = lambda ri, fa, which: rows[base + ((ri * 2 + fa) * 2 + which) * excite :][:excite]
            for which in range(2):
                comp = SETS[which][c]
                kind = 0 if comp < 3 else 2
                a_re = alpha_ref[kind, w : w + 1]
                a_im = alpha_ref[kind + 1, w : w + 1]
                f_re, f_im = pick(0, 0, which), pick(1, 0, which)
                if comp == 2:
                    f_re, f_im = -f_re, -f_im
                fwd_ref[w, 0, comp] = dip_ref[w, 0, comp].astype(jnp.float32) - (a_re * f_re - a_im * f_im)
                fwd_ref[w, 1, comp] = dip_ref[w, 1, comp].astype(jnp.float32) - (a_re * f_im + a_im * f_re)
                b_re, b_im = pick(0, 1, which), -pick(1, 1, which)
                if comp == 5:
                    b_re, b_im = -b_re, -b_im
                out_ref[w, 0, comp] = adj_ref[w, 0, comp].astype(jnp.float32) - b_re
                out_ref[w, 1, comp] = adj_ref[w, 1, comp].astype(jnp.float32) - b_im


def vmem(count):
    return [pl.BlockSpec(memory_space=pltpu.VMEM)] * count


def per_device(lattice, material, polarizability, wavenumber, dipoles, adjoint_in):
    n_tgt, n_src = lax.axis_size("tgt"), lax.axis_size("src")
    depth = n_tgt // BANDS
    waves, excite, atoms = dipoles.shape[0], dipoles.shape[3], dipoles.shape[4]
    kinds = polarizability.shape[0]
    width = waves * 24 * excite
    payload, alpha = pl.pallas_call(
        pack_kernel,
        in_specs=vmem(5),
        out_specs=vmem(2),
        out_shape=(
            jax.ShapeDtypeStruct((atoms, width), jnp.bfloat16),
            jax.ShapeDtypeStruct((kinds, waves, atoms), jnp.float32),
        ),
        name="pack",
    )(lattice, material.reshape(1, atoms), jnp.transpose(polarizability, (0, 2, 1)), dipoles, adjoint_in)
    tiles = [payload] + [
        lax.ppermute(payload, AXES, pairs(n_tgt, n_src, k, 0, 0)) for k in range(1, depth)
    ]
    kernels = pl.pallas_call(
        functools.partial(green_kernel, n_tgt=n_tgt, n_src=n_src),
        in_specs=[pl.BlockSpec(memory_space=pltpu.SMEM)],
        out_specs=pl.BlockSpec(memory_space=pltpu.VMEM),
        out_shape=jax.ShapeDtypeStruct((waves, 6, 2 * depth * atoms, 3 * BANDS * atoms), jnp.bfloat16),
        name="green",
    )(wavenumber)
    own, sent = pl.pallas_call(
        field_kernel,
        in_specs=vmem(depth + 1),
        out_specs=vmem(2),
        out_shape=(
            jax.ShapeDtypeStruct((atoms, width), jnp.float32),
            jax.ShapeDtypeStruct((3 * BANDS - 1, atoms, width), jnp.bfloat16),
        ),
        name="fields",
    )(*tiles, kernels)
    got = []
    for index in range(3 * BANDS - 1):
        slot, flip = divmod(index + 1, BANDS)
        got.append(lax.ppermute(sent[index], AXES, pairs(n_tgt, n_src, 0, flip, slot)))
    return pl.pallas_call(
        finish_kernel,
        in_specs=vmem(5 + len(got)),
        out_specs=vmem(2),
        out_shape=(
            jax.ShapeDtypeStruct(dipoles.shape, jnp.float32),
            jax.ShapeDtypeStruct(dipoles.shape, jnp.float32),
        ),
        name="finish",
    )(lattice, alpha, dipoles, adjoint_in, own, *got)


def solution(mesh):
    split = P(None, None, None, None, AXES)
    return jax.shard_map(
        per_device,
        mesh=mesh,
        in_specs=(P(None, AXES), P(AXES), P(), P(), split, split),
        out_specs=(split, split),
        check_vma=False,
    )
```

```python
import functools

import jax
import jax.numpy as jnp
from jax import lax
from jax.experimental import pallas as pl
from jax.experimental.pallas import tpu as pltpu
from jax.sharding import PartitionSpec as P

TILE_Y = 16
TILE_X = 2
ATOMS = TILE_X * TILE_Y
AXES = ("tgt", "src")
BANDS = 2

SETS = ((0, 1, 5), (3, 4, 2))
PLACES = (((0, 0),), ((1, 1),), ((2, 2),), ((1, 0), (0, 1)), ((2, 0), (0, 2)), ((2, 1), (1, 2)))


def z_partner(z, shift, count):
    return z ^ shift if count & (count - 1) == 0 else (z + shift) % count


def column_partner(s, slot, count):
    if slot == 0:
        return s
    if count % 2:
        return (s + (1 if slot == 1 else -1)) % count
    step = 1 if (s % 2 == 0) == (slot == 1) else -1
    return (s + step) % count


def pairs(n_tgt, n_src, shift, flip, slot):
    depth = n_tgt // BANDS
    out = []
    for t in range(n_tgt):
        z, y = divmod(t, BANDS)
        for s in range(n_src):
            to_t = z_partner(z, shift, depth) * BANDS + (y + flip) % BANDS
            out.append((t * n_src + s, to_t * n_src + column_partner(s, slot, n_src)))
    return out


def site_of(lattice):
    return (lattice[0:1] % TILE_X) * TILE_Y + lattice[1:2] % TILE_Y


def pack_kernel(*refs):
    sources, (payload_ref, alpha_ref, waves_ref, place_ref), scratch = refs[:6], refs[6:10], refs[10:]
    copies = [pltpu.make_async_copy(source, there, scratch[-1].at[i]) for i, (source, there) in enumerate(zip(sources, scratch))]
    for copy in copies:
        copy.start()
    for copy in copies:
        copy.wait()
    lattice_ref, material_ref, pol_ref, wave_ref, dip_ref, adj_ref = scratch[:6]
    waves, _, _, excite, atoms = dip_ref.shape
    types = pol_ref.shape[2]
    for w in range(waves):
        waves_ref[w : w + 1] = jnp.broadcast_to(wave_ref[0:1, w : w + 1], (1, waves_ref.shape[1]))
    place_ref[...] = jnp.broadcast_to(lattice_ref[:, 0:1], place_ref.shape)
    kinds = lax.broadcasted_iota(jnp.int32, (types, atoms), 0)
    onehot = jnp.where(kinds == material_ref[...], 1.0, 0.0).astype(jnp.float32)
    alpha = []
    for kind in range(4):
        value = jnp.dot(
            pol_ref[kind], onehot, precision=lax.Precision.HIGHEST, preferred_element_type=jnp.float32
        )
        alpha_ref[kind] = value
        alpha.append(value)
    rows = []
    for w in range(waves):
        fwd = {}
        adj = {}
        for comp in range(6):
            base = 0 if comp < 3 else 2
            a_re = alpha[base][w : w + 1]
            a_im = alpha[base + 1][w : w + 1]
            v_re = adj_ref[w, 0, comp].astype(jnp.float32)
            v_im = adj_ref[w, 1, comp].astype(jnp.float32)
            fwd[comp] = (dip_ref[w, 0, comp].astype(jnp.float32), dip_ref[w, 1, comp].astype(jnp.float32))
            adj[comp] = (a_re * v_re + a_im * v_im, a_re * v_im - a_im * v_re)
        for c in range(3):
            first, second = SETS[0][c], SETS[1][c]
            for ri in range(2):
                f1 = fwd[first][ri]
                f2 = fwd[second][ri] if c < 2 else -fwd[second][ri]
                a1 = adj[first][ri]
                a2 = adj[second][ri]
                if ri == 1:
                    a1, a2 = -a1, -a2
                if c == 2:
                    a1 = -a1
                rows += [f1, f2, a1, a2]
    table = jnp.concatenate(rows, axis=0).astype(jnp.bfloat16)
    sites = lax.broadcasted_iota(jnp.int32, (atoms, atoms), 0)
    place = jnp.where(sites == site_of(lattice_ref[...]), 1.0, 0.0).astype(jnp.bfloat16)
    payload_ref[...] = lax.dot_general(
        place, table, (((1,), (1,)), ((), ())), preferred_element_type=jnp.float32
    ).astype(jnp.bfloat16)


def sin_cos(x):
    turns = jnp.floor(x * 0.6366197723675814 + 0.5)
    rest = ((x - turns * 1.5703125) - turns * 4.837512969970703125e-4) - turns * 7.54978995489188216e-8
    sq = rest * rest
    sin = rest + rest * sq * (-1.6666654611e-1 + sq * (8.3321608736e-3 - sq * 1.9515295891e-4))
    cos = 1.0 - 0.5 * sq + sq * sq * (4.166664568298827e-2 + sq * (-1.388731625493765e-3 + sq * 2.443315711809948e-5))
    quarter = turns.astype(jnp.int32)
    odd = (quarter & 1) == 1
    sin, cos = jnp.where(odd, cos, sin), jnp.where(odd, sin, cos)
    sin = jnp.where((quarter & 2) == 2, -sin, sin)
    cos = jnp.where(((quarter + 1) & 2) == 2, -cos, cos)
    return sin, cos


def green_kernel(wave_ref, place_ref, out_ref, *, n_tgt, n_src):
    waves, _, double, targets = out_ref.shape
    sources = double // 2
    depth = n_tgt // BANDS
    band = place_ref[0:1] // TILE_X
    column = place_ref[1:2] // TILE_Y
    z, y = band // BANDS, band % BANDS
    period = n_src * TILE_Y
    if n_src % 2:
        step = 1
    else:
        step = 1 - 2 * (column % 2)
    lane = lax.broadcasted_iota(jnp.int32, (1, targets), 1)
    slot = lane // (BANDS * ATOMS)
    offset = jnp.where(slot == 0, 0, jnp.where(slot == 1, step, -step))
    to_band = z * BANDS + (y + lane // ATOMS) % BANDS
    to_x = to_band * TILE_X + lane % ATOMS // TILE_Y
    to_y = offset * TILE_Y + lane % TILE_Y
    for k in range(depth):
        from_band = z_partner(z, k, depth) * BANDS + y
        row = lax.broadcasted_iota(jnp.int32, (ATOMS, 1), 0)
        dx = to_x - (from_band * TILE_X + row // TILE_Y)
        dy = to_y - row % TILE_Y
        dy = jnp.where(2 * dy > period, dy - period, jnp.where(2 * dy < -period, dy + period, dy))
        dx = dx.astype(jnp.float32)
        dy = dy.astype(jnp.float32)
        square = dx * dx + dy * dy
        inverse = jnp.where(square > 0.5, lax.rsqrt(jnp.maximum(square, 1.0)), 0.0)
        radius = square * inverse
        ux = dx * inverse
        uy = dy * inverse
        xx, yy, xy = ux * ux, uy * uy, ux * uy
        ux = -ux
        for w in range(waves):
            wave = wave_ref[w : w + 1]
            sin, cos = sin_cos(wave * radius)
            inv = inverse * (1.0 / wave)
            g_re = cos * inv
            g_im = sin * inv
            h_re = g_re * inv
            h_im = g_im * inv
            e_re = h_re * inv + h_im
            e_im = h_im * inv - h_re
            near = (g_re - e_re, g_im - e_im)
            far = (3.0 * e_re - g_re, 3.0 * e_im - g_im)
            cross = (g_re - h_im, g_im + h_re)
            for part in range(2):
                there = pl.ds(part * sources + k * ATOMS, ATOMS)
                n, f, c = near[part], far[part], cross[part]
                out_ref[w, 0, there] = (n + f * xx).astype(jnp.bfloat16)
                out_ref[w, 1, there] = (n + f * yy).astype(jnp.bfloat16)
                out_ref[w, 2, there] = n.astype(jnp.bfloat16)
                out_ref[w, 3, there] = (f * xy).astype(jnp.bfloat16)
                out_ref[w, 4, there] = (c * uy).astype(jnp.bfloat16)
                out_ref[w, 5, there] = (c * ux).astype(jnp.bfloat16)


def field_kernel(*refs):
    *tile_refs, kernels_ref, own_ref, core_ref, flip_ref, side_ref, cross_ref = refs
    waves = kernels_ref.shape[0]
    gathered = jnp.concatenate([ref[...].astype(jnp.float32) for ref in tile_refs], axis=0)
    rows = gathered.T.astype(jnp.bfloat16)
    half = rows.shape[0] // (waves * 6)
    fields = []
    for w in range(waves):
        left = []
        for c in range(3):
            base = (w * 3 + c) * 2 * half
            re, im = rows[base : base + half], rows[base + half : base + 2 * half]
            left.append(
                jnp.concatenate(
                    [jnp.concatenate([re, -im], axis=1), jnp.concatenate([im, re], axis=1)], axis=0
                )
            )
        total = [None] * 3
        for index, places in enumerate(PLACES):
            stacked = jnp.concatenate([left[c_in] for c_in, _ in places], axis=0)
            product = jnp.dot(stacked, kernels_ref[w, index], preferred_element_type=jnp.float32)
            for number, (_, c_out) in enumerate(places):
                piece = product[number * 2 * half : (number + 1) * 2 * half]
                total[c_out] = piece if total[c_out] is None else total[c_out] + piece
        fields += total
    turned = jnp.concatenate(fields, axis=0).T
    piece = lambda slot, flip: turned[(slot * BANDS + flip) * ATOMS :][:ATOMS]
    own_ref[...] = piece(0, 0)
    core_ref[...] = piece(1, 0)
    flip_ref[0] = piece(0, 1).astype(jnp.bfloat16)
    flip_ref[1] = piece(1, 1).astype(jnp.bfloat16)
    side_ref[...] = piece(2, 0).astype(jnp.bfloat16)
    cross_ref[...] = piece(2, 1).astype(jnp.bfloat16)


def finish_kernel(*refs):
    lattice_ref, alpha_ref, dip_ref, adj_ref, own_ref, *rest = refs
    flip_ref, *got_refs, fwd_ref, out_ref = rest
    waves, _, _, excite, atoms = dip_ref.shape
    field = own_ref[...] + flip_ref[0].astype(jnp.float32)
    for ref in got_refs:
        field = field + ref[...].astype(jnp.float32)
    high = field.astype(jnp.bfloat16)
    low = (field - high.astype(jnp.float32)).astype(jnp.bfloat16)
    sites = lax.broadcasted_iota(jnp.int32, (atoms, atoms), 0)
    place = jnp.where(sites == site_of(lattice_ref[...]), 1.0, 0.0).astype(jnp.bfloat16)
    rows = lax.dot_general(
        jnp.concatenate([high, low], axis=0),
        jnp.concatenate([place, place], axis=0),
        (((0,), (0,)), ((), ())),
        preferred_element_type=jnp.float32,
    )
    for w in range(waves):
        for c in range(3):
            base = (w * 3 + c) * 8 * excite
            pick = lambda ri, fa, which: rows[base + ((ri * 2 + fa) * 2 + which) * excite :][:excite]
            for which in range(2):
                comp = SETS[which][c]
                kind = 0 if comp < 3 else 2
                a_re = alpha_ref[kind, w : w + 1]
                a_im = alpha_ref[kind + 1, w : w + 1]
                f_re, f_im = pick(0, 0, which), pick(1, 0, which)
                if comp == 2:
                    f_re, f_im = -f_re, -f_im
                fwd_ref[w, 0, comp] = dip_ref[w, 0, comp].astype(jnp.float32) - (a_re * f_re - a_im * f_im)
                fwd_ref[w, 1, comp] = dip_ref[w, 1, comp].astype(jnp.float32) - (a_re * f_im + a_im * f_re)
                b_re, b_im = pick(0, 1, which), -pick(1, 1, which)
                if comp == 5:
                    b_re, b_im = -b_re, -b_im
                out_ref[w, 0, comp] = adj_ref[w, 0, comp].astype(jnp.float32) - b_re
                out_ref[w, 1, comp] = adj_ref[w, 1, comp].astype(jnp.float32) - b_im


def vmem(count):
    return [pl.BlockSpec(memory_space=pltpu.VMEM)] * count


def per_device(lattice, material, polarizability, wavenumber, dipoles, adjoint_in):
    n_tgt, n_src = lax.axis_size("tgt"), lax.axis_size("src")
    depth = n_tgt // BANDS
    waves, excite, atoms = dipoles.shape[0], dipoles.shape[3], dipoles.shape[4]
    kinds = polarizability.shape[0]
    width = waves * 24 * excite
    arguments = (
        lattice,
        material.reshape(1, atoms),
        jnp.transpose(polarizability, (0, 2, 1)),
        wavenumber.reshape(1, waves),
        dipoles,
        adjoint_in,
    )
    targets = 3 * BANDS * atoms
    payload, alpha, wave_rows, place = pl.pallas_call(
        pack_kernel,
        in_specs=[pl.BlockSpec(memory_space=pltpu.HBM)] * len(arguments),
        out_specs=vmem(4),
        out_shape=(
            jax.ShapeDtypeStruct((atoms, width), jnp.bfloat16),
            jax.ShapeDtypeStruct((kinds, waves, atoms), jnp.float32),
            jax.ShapeDtypeStruct((waves, targets), jnp.float32),
            jax.ShapeDtypeStruct((2, targets), jnp.int32),
        ),
        scratch_shapes=[pltpu.VMEM(x.shape, x.dtype) for x in arguments]
        + [pltpu.SemaphoreType.DMA((len(arguments),))],
        compiler_params=pltpu.CompilerParams(vmem_limit_bytes=4 << 20),
        name="pack",
    )(*(pltpu.with_memory_space_constraint(x, pltpu.HBM) for x in arguments))
    send = lambda x, shift, flip, slot: lax.ppermute(x, AXES, pairs(n_tgt, n_src, shift, flip, slot))
    tiles = [payload] + [send(payload, k, 0, 0) for k in range(1, depth)]
    kernels = pl.pallas_call(
        functools.partial(green_kernel, n_tgt=n_tgt, n_src=n_src),
        in_specs=vmem(2),
        out_specs=pl.BlockSpec(memory_space=pltpu.VMEM),
        out_shape=jax.ShapeDtypeStruct((waves, 6, 2 * depth * atoms, targets), jnp.bfloat16),
        compiler_params=pltpu.CompilerParams(vmem_limit_bytes=12 << 20),
        name="green",
    )(wave_rows, place)
    tile = jax.ShapeDtypeStruct((atoms, width), jnp.bfloat16)
    wide = jax.ShapeDtypeStruct((atoms, width), jnp.float32)
    own, core, flip, side, cross = pl.pallas_call(
        field_kernel,
        in_specs=vmem(depth + 1),
        out_specs=vmem(5),
        out_shape=(wide, wide, jax.ShapeDtypeStruct((2, atoms, width), jnp.bfloat16), tile, tile),
        compiler_params=pltpu.CompilerParams(vmem_limit_bytes=12 << 20),
        name="fields",
    )(*tiles, kernels)
    cross = send(cross, 0, 1, 2)
    side = send(side, 0, 0, 2)
    flip = send(flip, 0, 1, 0)
    core = send((core + flip[1].astype(jnp.float32)).astype(jnp.bfloat16), 0, 0, 1)
    got = (flip, side, cross, core)
    return pl.pallas_call(
        finish_kernel,
        in_specs=vmem(5 + len(got)),
        out_specs=vmem(2),
        out_shape=(
            jax.ShapeDtypeStruct(dipoles.shape, jnp.float32),
            jax.ShapeDtypeStruct(dipoles.shape, jnp.float32),
        ),
        compiler_params=pltpu.CompilerParams(vmem_limit_bytes=8 << 20),
        name="finish",
    )(lattice, alpha, dipoles, adjoint_in, own, *got)


def solution(mesh):
    split = P(None, None, None, None, AXES)
    return jax.shard_map(
        per_device,
        mesh=mesh,
        in_specs=(P(None, AXES), P(AXES), P(), P(), split, split),
        out_specs=(split, split),
        check_vma=False,
    )
```

```python
import functools

import jax
import jax.numpy as jnp
from jax import lax
from jax.experimental import pallas as pl
from jax.experimental.pallas import tpu as pltpu
from jax.sharding import PartitionSpec as P

TILE_Y = 16
TILE_X = 2
ATOMS = TILE_X * TILE_Y
AXES = ("tgt", "src")
BANDS = 2

SETS = ((0, 1, 5), (3, 4, 2))
PLACES = (((0, 0),), ((1, 1),), ((2, 2),), ((1, 0), (0, 1)), ((2, 0), (0, 2)), ((2, 1), (1, 2)))


def z_partner(z, shift, count):
    return z ^ shift if count & (count - 1) == 0 else (z + shift) % count


def column_partner(s, slot, count):
    if slot == 0:
        return s
    if count % 2:
        return (s + (1 if slot == 1 else -1)) % count
    step = 1 if (s % 2 == 0) == (slot == 1) else -1
    return (s + step) % count


def pairs(n_tgt, n_src, shift, flip, slot):
    depth = n_tgt // BANDS
    out = []
    for t in range(n_tgt):
        z, y = divmod(t, BANDS)
        for s in range(n_src):
            to_t = z_partner(z, shift, depth) * BANDS + (y + flip) % BANDS
            out.append((t * n_src + s, to_t * n_src + column_partner(s, slot, n_src)))
    return out


def site_of(lattice):
    return (lattice[0:1] % TILE_X) * TILE_Y + lattice[1:2] % TILE_Y


def pack_kernel(*refs):
    sources, (payload_ref, alpha_ref, waves_ref, place_ref), scratch = refs[:6], refs[6:10], refs[10:]
    copies = [pltpu.make_async_copy(source, there, scratch[-1].at[i]) for i, (source, there) in enumerate(zip(sources, scratch))]
    for copy in copies:
        copy.start()
    for copy in copies:
        copy.wait()
    lattice_ref, material_ref, pol_ref, wave_ref, dip_ref, adj_ref = scratch[:6]
    waves, _, _, excite, atoms = dip_ref.shape
    types = pol_ref.shape[2]
    for w in range(waves):
        waves_ref[w : w + 1] = jnp.broadcast_to(wave_ref[0:1, w : w + 1], (1, waves_ref.shape[1]))
    place_ref[...] = jnp.broadcast_to(lattice_ref[:, 0:1], place_ref.shape)
    kinds = lax.broadcasted_iota(jnp.int32, (types, atoms), 0)
    onehot = jnp.where(kinds == material_ref[...], 1.0, 0.0).astype(jnp.float32)
    alpha = []
    for kind in range(4):
        value = jnp.dot(
            pol_ref[kind], onehot, precision=lax.Precision.HIGHEST, preferred_element_type=jnp.float32
        )
        alpha_ref[kind] = value
        alpha.append(value)
    rows = []
    for w in range(waves):
        fwd = {}
        adj = {}
        for comp in range(6):
            base = 0 if comp < 3 else 2
            a_re = alpha[base][w : w + 1]
            a_im = alpha[base + 1][w : w + 1]
            v_re = adj_ref[w, 0, comp].astype(jnp.float32)
            v_im = adj_ref[w, 1, comp].astype(jnp.float32)
            fwd[comp] = (dip_ref[w, 0, comp].astype(jnp.float32), dip_ref[w, 1, comp].astype(jnp.float32))
            adj[comp] = (a_re * v_re + a_im * v_im, a_re * v_im - a_im * v_re)
        for c in range(3):
            first, second = SETS[0][c], SETS[1][c]
            for ri in range(2):
                f1 = fwd[first][ri]
                f2 = fwd[second][ri] if c < 2 else -fwd[second][ri]
                a1 = adj[first][ri]
                a2 = adj[second][ri]
                if ri == 1:
                    a1, a2 = -a1, -a2
                if c == 2:
                    a1 = -a1
                rows += [f1, f2, a1, a2]
    table = jnp.concatenate(rows, axis=0).astype(jnp.bfloat16)
    sites = lax.broadcasted_iota(jnp.int32, (atoms, atoms), 0)
    place = jnp.where(sites == site_of(lattice_ref[...]), 1.0, 0.0).astype(jnp.bfloat16)
    payload_ref[...] = lax.dot_general(
        place, table, (((1,), (1,)), ((), ())), preferred_element_type=jnp.float32
    ).astype(jnp.bfloat16)


def sin_cos(x):
    turns = jnp.floor(x * 0.6366197723675814 + 0.5)
    rest = ((x - turns * 1.5703125) - turns * 4.837512969970703125e-4) - turns * 7.54978995489188216e-8
    sq = rest * rest
    sin = rest + rest * sq * (-1.6666654611e-1 + sq * (8.3321608736e-3 - sq * 1.9515295891e-4))
    cos = 1.0 - 0.5 * sq + sq * sq * (4.166664568298827e-2 + sq * (-1.388731625493765e-3 + sq * 2.443315711809948e-5))
    quarter = turns.astype(jnp.int32)
    odd = (quarter & 1) == 1
    sin, cos = jnp.where(odd, cos, sin), jnp.where(odd, sin, cos)
    sin = jnp.where((quarter & 2) == 2, -sin, sin)
    cos = jnp.where(((quarter + 1) & 2) == 2, -cos, cos)
    return sin, cos


def green_kernel(wave_ref, place_ref, out_ref, *, n_tgt, n_src):
    waves, _, double, targets = out_ref.shape
    sources = double // 2
    depth = n_tgt // BANDS
    band = place_ref[0:1] // TILE_X
    column = place_ref[1:2] // TILE_Y
    z, y = band // BANDS, band % BANDS
    period = n_src * TILE_Y
    if n_src % 2:
        step = 1
    else:
        step = 1 - 2 * (column % 2)
    lane = lax.broadcasted_iota(jnp.int32, (1, targets), 1)
    slot = lane // (BANDS * ATOMS)
    offset = jnp.where(slot == 0, 0, jnp.where(slot == 1, step, -step))
    to_band = z * BANDS + (y + lane // ATOMS) % BANDS
    to_x = to_band * TILE_X + lane % ATOMS // TILE_Y
    to_y = offset * TILE_Y + lane % TILE_Y
    for k in range(depth):
        from_band = z_partner(z, k, depth) * BANDS + y
        row = lax.broadcasted_iota(jnp.int32, (ATOMS, 1), 0)
        dx = to_x - (from_band * TILE_X + row // TILE_Y)
        dy = to_y - row % TILE_Y
        dy = jnp.where(2 * dy > period, dy - period, jnp.where(2 * dy < -period, dy + period, dy))
        dx = dx.astype(jnp.float32)
        dy = dy.astype(jnp.float32)
        square = dx * dx + dy * dy
        inverse = jnp.where(square > 0.5, lax.rsqrt(jnp.maximum(square, 1.0)), 0.0)
        radius = square * inverse
        ux = dx * inverse
        uy = dy * inverse
        xx, yy, xy = ux * ux, uy * uy, ux * uy
        ux = -ux
        for w in range(waves):
            wave = wave_ref[w : w + 1]
            sin, cos = sin_cos(wave * radius)
            inv = inverse * (1.0 / wave)
            g_re = cos * inv
            g_im = sin * inv
            h_re = g_re * inv
            h_im = g_im * inv
            e_re = h_re * inv + h_im
            e_im = h_im * inv - h_re
            near = (g_re - e_re, g_im - e_im)
            far = (3.0 * e_re - g_re, 3.0 * e_im - g_im)
            cross = (g_re - h_im, g_im + h_re)
            for part in range(2):
                there = pl.ds(part * sources + k * ATOMS, ATOMS)
                n, f, c = near[part], far[part], cross[part]
                out_ref[w, 0, there] = (n + f * xx).astype(jnp.bfloat16)
                out_ref[w, 1, there] = (n + f * yy).astype(jnp.bfloat16)
                out_ref[w, 2, there] = n.astype(jnp.bfloat16)
                out_ref[w, 3, there] = (f * xy).astype(jnp.bfloat16)
                out_ref[w, 4, there] = (c * uy).astype(jnp.bfloat16)
                out_ref[w, 5, there] = (c * ux).astype(jnp.bfloat16)


def field_kernel(*refs):
    *tile_refs, kernels_ref, own_ref, core_ref, flip_ref, side_ref, cross_ref = refs
    waves = kernels_ref.shape[0]
    gathered = jnp.concatenate([ref[...].astype(jnp.float32) for ref in tile_refs], axis=0)
    rows = gathered.T.astype(jnp.bfloat16)
    half = rows.shape[0] // (waves * 6)
    fields = []
    for w in range(waves):
        left = []
        for c in range(3):
            base = (w * 3 + c) * 2 * half
            re, im = rows[base : base + half], rows[base + half : base + 2 * half]
            left.append(
                jnp.concatenate(
                    [jnp.concatenate([re, -im], axis=1), jnp.concatenate([im, re], axis=1)], axis=0
                )
            )
        total = [None] * 3
        for index, places in enumerate(PLACES):
            stacked = jnp.concatenate([left[c_in] for c_in, _ in places], axis=0)
            product = jnp.dot(stacked, kernels_ref[w, index], preferred_element_type=jnp.float32)
            for number, (_, c_out) in enumerate(places):
                piece = product[number * 2 * half : (number + 1) * 2 * half]
                total[c_out] = piece if total[c_out] is None else total[c_out] + piece
        fields += total
    turned = jnp.concatenate(fields, axis=0).T
    piece = lambda slot, flip: turned[(slot * BANDS + flip) * ATOMS :][:ATOMS]
    own_ref[...] = piece(0, 0)
    core_ref[...] = piece(1, 0)
    flip_ref[0] = piece(0, 1).astype(jnp.bfloat16)
    flip_ref[1] = piece(1, 1).astype(jnp.bfloat16)
    side_ref[...] = piece(2, 0).astype(jnp.bfloat16)
    cross_ref[...] = piece(2, 1).astype(jnp.bfloat16)


def finish_kernel(*refs):
    lattice_ref, alpha_ref, dip_ref, adj_ref, own_ref, *rest = refs
    *got_refs, fwd_ref, out_ref = rest
    flip_ref = got_refs.pop(2)
    waves, _, _, excite, atoms = dip_ref.shape
    field = own_ref[...] + flip_ref[0].astype(jnp.float32)
    for ref in got_refs:
        field = field + ref[...].astype(jnp.float32)
    high = field.astype(jnp.bfloat16)
    low = (field - high.astype(jnp.float32)).astype(jnp.bfloat16)
    sites = lax.broadcasted_iota(jnp.int32, (atoms, atoms), 0)
    place = jnp.where(sites == site_of(lattice_ref[...]), 1.0, 0.0).astype(jnp.bfloat16)
    rows = lax.dot_general(
        jnp.concatenate([high, low], axis=0),
        jnp.concatenate([place, place], axis=0),
        (((0,), (0,)), ((), ())),
        preferred_element_type=jnp.float32,
    )
    for w in range(waves):
        for c in range(3):
            base = (w * 3 + c) * 8 * excite
            pick = lambda ri, fa, which: rows[base + ((ri * 2 + fa) * 2 + which) * excite :][:excite]
            for which in range(2):
                comp = SETS[which][c]
                kind = 0 if comp < 3 else 2
                a_re = alpha_ref[kind, w : w + 1]
                a_im = alpha_ref[kind + 1, w : w + 1]
                f_re, f_im = pick(0, 0, which), pick(1, 0, which)
                if comp == 2:
                    f_re, f_im = -f_re, -f_im
                fwd_ref[w, 0, comp] = dip_ref[w, 0, comp].astype(jnp.float32) - (a_re * f_re - a_im * f_im)
                fwd_ref[w, 1, comp] = dip_ref[w, 1, comp].astype(jnp.float32) - (a_re * f_im + a_im * f_re)
                b_re, b_im = pick(0, 1, which), -pick(1, 1, which)
                if comp == 5:
                    b_re, b_im = -b_re, -b_im
                out_ref[w, 0, comp] = adj_ref[w, 0, comp].astype(jnp.float32) - b_re
                out_ref[w, 1, comp] = adj_ref[w, 1, comp].astype(jnp.float32) - b_im


def vmem(count):
    return [pl.BlockSpec(memory_space=pltpu.VMEM)] * count


def per_device(lattice, material, polarizability, wavenumber, dipoles, adjoint_in):
    n_tgt, n_src = lax.axis_size("tgt"), lax.axis_size("src")
    depth = n_tgt // BANDS
    waves, excite, atoms = dipoles.shape[0], dipoles.shape[3], dipoles.shape[4]
    kinds = polarizability.shape[0]
    width = waves * 24 * excite
    arguments = (
        lattice,
        material.reshape(1, atoms),
        jnp.transpose(polarizability, (0, 2, 1)),
        wavenumber.reshape(1, waves),
        dipoles,
        adjoint_in,
    )
    targets = 3 * BANDS * atoms
    payload, alpha, wave_rows, place = pl.pallas_call(
        pack_kernel,
        in_specs=[pl.BlockSpec(memory_space=pltpu.HBM)] * len(arguments),
        out_specs=vmem(4),
        out_shape=(
            jax.ShapeDtypeStruct((atoms, width), jnp.bfloat16),
            jax.ShapeDtypeStruct((kinds, waves, atoms), jnp.float32),
            jax.ShapeDtypeStruct((waves, targets), jnp.float32),
            jax.ShapeDtypeStruct((2, targets), jnp.int32),
        ),
        scratch_shapes=[pltpu.VMEM(x.shape, x.dtype) for x in arguments]
        + [pltpu.SemaphoreType.DMA((len(arguments),))],
        compiler_params=pltpu.CompilerParams(vmem_limit_bytes=4 << 20),
        name="pack",
    )(*(pltpu.with_memory_space_constraint(x, pltpu.HBM) for x in arguments))
    send = lambda x, shift, flip, slot: lax.ppermute(x, AXES, pairs(n_tgt, n_src, shift, flip, slot))
    tiles = [payload] + [send(payload, k, 0, 0) for k in range(1, depth)]
    kernels = pl.pallas_call(
        functools.partial(green_kernel, n_tgt=n_tgt, n_src=n_src),
        in_specs=vmem(2),
        out_specs=pl.BlockSpec(memory_space=pltpu.VMEM),
        out_shape=jax.ShapeDtypeStruct((waves, 6, 2 * depth * atoms, targets), jnp.bfloat16),
        compiler_params=pltpu.CompilerParams(vmem_limit_bytes=12 << 20),
        name="green",
    )(wave_rows, place)
    tile = jax.ShapeDtypeStruct((atoms, width), jnp.bfloat16)
    wide = jax.ShapeDtypeStruct((atoms, width), jnp.float32)
    own, core, flip, side, cross = pl.pallas_call(
        field_kernel,
        in_specs=vmem(depth + 1),
        out_specs=vmem(5),
        out_shape=(wide, wide, jax.ShapeDtypeStruct((2, atoms, width), jnp.bfloat16), tile, tile),
        compiler_params=pltpu.CompilerParams(vmem_limit_bytes=12 << 20),
        name="fields",
    )(*tiles, kernels)
    cross = send(cross, 0, 1, 2)
    side = send(side, 0, 0, 2)
    flip = send(flip, 0, 1, 0)
    core = send((core + flip[1].astype(jnp.float32)).astype(jnp.bfloat16), 0, 0, 1)
    got = (cross, side, flip, core)
    return pl.pallas_call(
        finish_kernel,
        in_specs=vmem(5 + len(got)),
        out_specs=vmem(2),
        out_shape=(
            jax.ShapeDtypeStruct(dipoles.shape, jnp.float32),
            jax.ShapeDtypeStruct(dipoles.shape, jnp.float32),
        ),
        compiler_params=pltpu.CompilerParams(vmem_limit_bytes=8 << 20),
        name="finish",
    )(lattice, alpha, dipoles, adjoint_in, own, *got)


def solution(mesh):
    split = P(None, None, None, None, AXES)
    return jax.shard_map(
        per_device,
        mesh=mesh,
        in_specs=(P(None, AXES), P(AXES), P(), P(), split, split),
        out_specs=(split, split),
        check_vma=False,
    )
```

```python
import functools

import jax
import jax.numpy as jnp
from jax import lax
from jax.experimental import pallas as pl
from jax.experimental.pallas import tpu as pltpu
from jax.sharding import PartitionSpec as P

TILE_Y = 16
TILE_X = 2
ATOMS = TILE_X * TILE_Y
AXES = ("tgt", "src")
BANDS = 2

SETS = ((0, 1, 5), (3, 4, 2))
PLACES = (((0, 0),), ((1, 1),), ((2, 2),), ((1, 0), (0, 1)), ((2, 0), (0, 2)), ((2, 1), (1, 2)))


def z_partner(z, shift, count):
    return z ^ shift if count & (count - 1) == 0 else (z + shift) % count


def column_partner(s, slot, count):
    if slot == 0:
        return s
    if count % 2:
        return (s + (1 if slot == 1 else -1)) % count
    step = 1 if (s % 2 == 0) == (slot == 1) else -1
    return (s + step) % count


def pairs(n_tgt, n_src, shift, flip, slot):
    depth = n_tgt // BANDS
    out = []
    for t in range(n_tgt):
        z, y = divmod(t, BANDS)
        for s in range(n_src):
            to_t = z_partner(z, shift, depth) * BANDS + (y + flip) % BANDS
            out.append((t * n_src + s, to_t * n_src + column_partner(s, slot, n_src)))
    return out


def site_of(lattice):
    return (lattice[0:1] % TILE_X) * TILE_Y + lattice[1:2] % TILE_Y


def pack_kernel(*refs):
    sources, (payload_ref, alpha_ref, waves_ref, place_ref), scratch = refs[:6], refs[6:10], refs[10:]
    copies = [pltpu.make_async_copy(source, there, scratch[-1].at[i]) for i, (source, there) in enumerate(zip(sources, scratch))]
    for copy in reversed(copies):
        copy.start()
    for copy in copies[:4]:
        copy.wait()
    lattice_ref, material_ref, pol_ref, wave_ref, dip_ref, adj_ref = scratch[:6]
    waves, _, _, excite, atoms = dip_ref.shape
    types = pol_ref.shape[2]
    for w in range(waves):
        waves_ref[w : w + 1] = jnp.broadcast_to(wave_ref[0:1, w : w + 1], (1, waves_ref.shape[1]))
    place_ref[...] = jnp.broadcast_to(lattice_ref[:, 0:1], place_ref.shape)
    kinds = lax.broadcasted_iota(jnp.int32, (types, atoms), 0)
    onehot = jnp.where(kinds == material_ref[...], 1.0, 0.0).astype(jnp.float32)
    rest = jnp.concatenate([pol_ref[kind] for kind in range(4)], axis=0)
    parts = []
    for _ in range(3):
        part = rest.astype(jnp.bfloat16)
        rest = rest - part.astype(jnp.float32)
        parts.append(part)
    onehot = onehot.astype(jnp.bfloat16)
    table = jnp.dot(
        jnp.concatenate(parts, axis=1),
        jnp.concatenate([onehot] * 3, axis=0),
        preferred_element_type=jnp.float32,
    )
    alpha = [table[kind * waves : (kind + 1) * waves] for kind in range(4)]
    for kind in range(4):
        alpha_ref[kind] = alpha[kind]
    for copy in copies[4:]:
        copy.wait()
    rows = []
    for w in range(waves):
        fwd = {}
        adj = {}
        for comp in range(6):
            base = 0 if comp < 3 else 2
            a_re = alpha[base][w : w + 1]
            a_im = alpha[base + 1][w : w + 1]
            v_re = adj_ref[w, 0, comp].astype(jnp.float32)
            v_im = adj_ref[w, 1, comp].astype(jnp.float32)
            fwd[comp] = (dip_ref[w, 0, comp].astype(jnp.float32), dip_ref[w, 1, comp].astype(jnp.float32))
            adj[comp] = (a_re * v_re + a_im * v_im, a_re * v_im - a_im * v_re)
        for c in range(3):
            first, second = SETS[0][c], SETS[1][c]
            for ri in range(2):
                f1 = fwd[first][ri]
                f2 = fwd[second][ri] if c < 2 else -fwd[second][ri]
                a1 = adj[first][ri]
                a2 = adj[second][ri]
                if ri == 1:
                    a1, a2 = -a1, -a2
                if c == 2:
                    a1 = -a1
                rows += [f1, f2, a1, a2]
    table = jnp.concatenate(rows, axis=0).astype(jnp.bfloat16)
    sites = lax.broadcasted_iota(jnp.int32, (atoms, atoms), 0)
    place = jnp.where(sites == site_of(lattice_ref[...]), 1.0, 0.0).astype(jnp.bfloat16)
    payload_ref[...] = lax.dot_general(
        place, table, (((1,), (1,)), ((), ())), preferred_element_type=jnp.float32
    ).astype(jnp.bfloat16)


def slot_groups(depth):
    order = [0] + list(range(depth - 1, 0, -1))
    half = depth // 2
    return order[:half], order[half:]


def kernel_row(k, part, depth):
    for number, group in enumerate(slot_groups(depth)):
        if k in group:
            return (2 * number * len(group) + part * len(group) + group.index(k)) * ATOMS


def sin_cos(x):
    turns = jnp.floor(x * 0.6366197723675814 + 0.5)
    rest = ((x - turns * 1.5703125) - turns * 4.837512969970703125e-4) - turns * 7.54978995489188216e-8
    sq = rest * rest
    sin = rest + rest * sq * (-1.6666654611e-1 + sq * (8.3321608736e-3 - sq * 1.9515295891e-4))
    cos = 1.0 - 0.5 * sq + sq * sq * (4.166664568298827e-2 + sq * (-1.388731625493765e-3 + sq * 2.443315711809948e-5))
    quarter = turns.astype(jnp.int32)
    odd = (quarter & 1) == 1
    sin, cos = jnp.where(odd, cos, sin), jnp.where(odd, sin, cos)
    sin = jnp.where((quarter & 2) == 2, -sin, sin)
    cos = jnp.where(((quarter + 1) & 2) == 2, -cos, cos)
    return sin, cos


def green_kernel(wave_ref, place_ref, out_ref, *, n_tgt, n_src):
    waves, _, _, targets = out_ref.shape
    depth = n_tgt // BANDS
    band = place_ref[0:1] // TILE_X
    column = place_ref[1:2] // TILE_Y
    z, y = band // BANDS, band % BANDS
    period = n_src * TILE_Y
    if n_src % 2:
        step = 1
    else:
        step = 1 - 2 * (column % 2)
    lane = lax.broadcasted_iota(jnp.int32, (1, targets), 1)
    slot = lane // (BANDS * ATOMS)
    offset = jnp.where(slot == 0, 0, jnp.where(slot == 1, step, -step))
    to_band = z * BANDS + (y + lane // ATOMS) % BANDS
    to_x = to_band * TILE_X + lane % ATOMS // TILE_Y
    to_y = offset * TILE_Y + lane % TILE_Y
    for k in range(depth):
        from_band = z_partner(z, k, depth) * BANDS + y
        row = lax.broadcasted_iota(jnp.int32, (ATOMS, 1), 0)
        dx = to_x - (from_band * TILE_X + row // TILE_Y)
        dy = to_y - row % TILE_Y
        dy = jnp.where(2 * dy > period, dy - period, jnp.where(2 * dy < -period, dy + period, dy))
        dx = dx.astype(jnp.float32)
        dy = dy.astype(jnp.float32)
        square = dx * dx + dy * dy
        inverse = jnp.where(square > 0.5, lax.rsqrt(jnp.maximum(square, 1.0)), 0.0)
        radius = square * inverse
        ux = dx * inverse
        uy = dy * inverse
        xx, yy, xy = ux * ux, uy * uy, ux * uy
        ux = -ux
        for w in range(waves):
            wave = wave_ref[w : w + 1]
            sin, cos = sin_cos(wave * radius)
            inv = inverse * (1.0 / wave)
            g_re = cos * inv
            g_im = sin * inv
            h_re = g_re * inv
            h_im = g_im * inv
            e_re = h_re * inv + h_im
            e_im = h_im * inv - h_re
            near = (g_re - e_re, g_im - e_im)
            far = (3.0 * e_re - g_re, 3.0 * e_im - g_im)
            cross = (g_re - h_im, g_im + h_re)
            for part in range(2):
                there = pl.ds(kernel_row(k, part, depth), ATOMS)
                n, f, c = near[part], far[part], cross[part]
                out_ref[w, 0, there] = (n + f * xx).astype(jnp.bfloat16)
                out_ref[w, 1, there] = (n + f * yy).astype(jnp.bfloat16)
                out_ref[w, 2, there] = n.astype(jnp.bfloat16)
                out_ref[w, 3, there] = (f * xy).astype(jnp.bfloat16)
                out_ref[w, 4, there] = (c * uy).astype(jnp.bfloat16)
                out_ref[w, 5, there] = (c * ux).astype(jnp.bfloat16)


def group_fields(tile_refs, kernels_ref, group):
    waves = kernels_ref.shape[0]
    count = len(tile_refs) * ATOMS
    once = jnp.concatenate([ref[...] for ref in tile_refs], axis=0)
    rows = jnp.concatenate([once, once], axis=0).astype(jnp.float32).T
    first = lax.broadcasted_iota(jnp.int32, (1, 2 * count), 1) < count
    half = rows.shape[0] // (waves * 6)
    fields = []
    for w in range(waves):
        left = []
        for c in range(3):
            base = (w * 3 + c) * 2 * half
            re, im = rows[base : base + half], rows[base + half : base + 2 * half]
            both = [jnp.where(first, re, -im), jnp.where(first, im, re)]
            left.append(jnp.concatenate(both, axis=0).astype(jnp.bfloat16))
        total = [None] * 3
        for index, places in enumerate(PLACES):
            stacked = jnp.concatenate([left[c_in] for c_in, _ in places], axis=0)
            chosen = kernels_ref[w, index, 2 * group * count : 2 * (group + 1) * count]
            product = jnp.dot(stacked, chosen, preferred_element_type=jnp.float32)
            for number, (_, c_out) in enumerate(places):
                there = product[number * 2 * half : (number + 1) * 2 * half]
                total[c_out] = there if total[c_out] is None else total[c_out] + there
        fields += total
    return jnp.concatenate(fields, axis=0)


def early_kernel(*refs):
    *tile_refs, kernels_ref, sum_ref = refs
    sum_ref[...] = group_fields(tile_refs, kernels_ref, 0)


def late_kernel(*refs):
    *tile_refs, kernels_ref, sum_ref, own_ref, core_ref, flip_ref, side_ref, cross_ref = refs
    turned = (group_fields(tile_refs, kernels_ref, 1) + sum_ref[...]).T
    piece = lambda slot, flip: turned[(slot * BANDS + flip) * ATOMS :][:ATOMS]
    own_ref[...] = piece(0, 0)
    core_ref[...] = piece(1, 0)
    flip_ref[0] = piece(0, 1).astype(jnp.bfloat16)
    flip_ref[1] = piece(1, 1).astype(jnp.bfloat16)
    side_ref[...] = piece(2, 0).astype(jnp.bfloat16)
    cross_ref[...] = piece(2, 1).astype(jnp.bfloat16)


def finish_kernel(*refs):
    lattice_ref, alpha_ref, dip_ref, adj_ref, own_ref, *rest = refs
    *got_refs, fwd_ref, out_ref = rest
    flip_ref = got_refs.pop(2)
    waves, _, _, excite, atoms = dip_ref.shape
    field = own_ref[...] + flip_ref[0].astype(jnp.float32)
    for ref in got_refs:
        field = field + ref[...].astype(jnp.float32)
    high = field.astype(jnp.bfloat16)
    low = (field - high.astype(jnp.float32)).astype(jnp.bfloat16)
    sites = lax.broadcasted_iota(jnp.int32, (atoms, atoms), 0)
    place = jnp.where(sites == site_of(lattice_ref[...]), 1.0, 0.0).astype(jnp.bfloat16)
    rows = lax.dot_general(
        jnp.concatenate([high, low], axis=0),
        jnp.concatenate([place, place], axis=0),
        (((0,), (0,)), ((), ())),
        preferred_element_type=jnp.float32,
    )
    for w in range(waves):
        for c in range(3):
            base = (w * 3 + c) * 8 * excite
            pick = lambda ri, fa, which: rows[base + ((ri * 2 + fa) * 2 + which) * excite :][:excite]
            for which in range(2):
                comp = SETS[which][c]
                kind = 0 if comp < 3 else 2
                a_re = alpha_ref[kind, w : w + 1]
                a_im = alpha_ref[kind + 1, w : w + 1]
                f_re, f_im = pick(0, 0, which), pick(1, 0, which)
                if comp == 2:
                    f_re, f_im = -f_re, -f_im
                fwd_ref[w, 0, comp] = dip_ref[w, 0, comp].astype(jnp.float32) - (a_re * f_re - a_im * f_im)
                fwd_ref[w, 1, comp] = dip_ref[w, 1, comp].astype(jnp.float32) - (a_re * f_im + a_im * f_re)
                b_re, b_im = pick(0, 1, which), -pick(1, 1, which)
                if comp == 5:
                    b_re, b_im = -b_re, -b_im
                out_ref[w, 0, comp] = adj_ref[w, 0, comp].astype(jnp.float32) - b_re
                out_ref[w, 1, comp] = adj_ref[w, 1, comp].astype(jnp.float32) - b_im


def vmem(count):
    return [pl.BlockSpec(memory_space=pltpu.VMEM)] * count


def per_device(lattice, material, polarizability, wavenumber, dipoles, adjoint_in):
    n_tgt, n_src = lax.axis_size("tgt"), lax.axis_size("src")
    depth = n_tgt // BANDS
    waves, excite, atoms = dipoles.shape[0], dipoles.shape[3], dipoles.shape[4]
    kinds = polarizability.shape[0]
    width = waves * 24 * excite
    arguments = (
        lattice,
        material.reshape(1, atoms),
        jnp.transpose(polarizability, (0, 2, 1)),
        wavenumber.reshape(1, waves),
        dipoles,
        adjoint_in,
    )
    targets = 3 * BANDS * atoms
    payload, alpha, wave_rows, place = pl.pallas_call(
        pack_kernel,
        in_specs=[pl.BlockSpec(memory_space=pltpu.HBM)] * len(arguments),
        out_specs=vmem(4),
        out_shape=(
            jax.ShapeDtypeStruct((atoms, width), jnp.bfloat16),
            jax.ShapeDtypeStruct((kinds, waves, atoms), jnp.float32),
            jax.ShapeDtypeStruct((waves, targets), jnp.float32),
            jax.ShapeDtypeStruct((2, targets), jnp.int32),
        ),
        scratch_shapes=[pltpu.VMEM(x.shape, x.dtype) for x in arguments]
        + [pltpu.SemaphoreType.DMA((len(arguments),))],
        compiler_params=pltpu.CompilerParams(vmem_limit_bytes=4 << 20),
        name="pack",
    )(*(pltpu.with_memory_space_constraint(x, pltpu.HBM) for x in arguments))
    send = lambda x, shift, flip, slot: lax.ppermute(x, AXES, pairs(n_tgt, n_src, shift, flip, slot))
    tiles = [payload] + [send(payload, k, 0, 0) for k in range(1, depth)]
    kernels = pl.pallas_call(
        functools.partial(green_kernel, n_tgt=n_tgt, n_src=n_src),
        in_specs=vmem(2),
        out_specs=pl.BlockSpec(memory_space=pltpu.VMEM),
        out_shape=jax.ShapeDtypeStruct((waves, 6, 2 * depth * atoms, targets), jnp.bfloat16),
        compiler_params=pltpu.CompilerParams(vmem_limit_bytes=12 << 20),
        name="green",
    )(wave_rows, place)
    tile = jax.ShapeDtypeStruct((atoms, width), jnp.bfloat16)
    wide = jax.ShapeDtypeStruct((atoms, width), jnp.float32)
    early, late = slot_groups(depth)
    early_sum = pl.pallas_call(
        early_kernel,
        in_specs=vmem(len(early) + 1),
        out_specs=pl.BlockSpec(memory_space=pltpu.VMEM),
        out_shape=jax.ShapeDtypeStruct((width, targets), jnp.float32),
        compiler_params=pltpu.CompilerParams(vmem_limit_bytes=12 << 20),
        name="early",
    )(*[tiles[k] for k in early], kernels)
    own, core, flip, side, cross = pl.pallas_call(
        late_kernel,
        in_specs=vmem(len(late) + 2),
        out_specs=vmem(5),
        out_shape=(wide, wide, jax.ShapeDtypeStruct((2, atoms, width), jnp.bfloat16), tile, tile),
        compiler_params=pltpu.CompilerParams(vmem_limit_bytes=12 << 20),
        name="late",
    )(*[tiles[k] for k in late], kernels, early_sum)
    cross = send(cross, 0, 1, 2)
    side = send(side, 0, 0, 2)
    flip = send(flip, 0, 1, 0)
    core = send((core + flip[1].astype(jnp.float32)).astype(jnp.bfloat16), 0, 0, 1)
    got = (cross, side, flip, core)
    return pl.pallas_call(
        finish_kernel,
        in_specs=vmem(5 + len(got)),
        out_specs=vmem(2),
        out_shape=(
            jax.ShapeDtypeStruct(dipoles.shape, jnp.float32),
            jax.ShapeDtypeStruct(dipoles.shape, jnp.float32),
        ),
        compiler_params=pltpu.CompilerParams(vmem_limit_bytes=8 << 20),
        name="finish",
    )(lattice, alpha, dipoles, adjoint_in, own, *got)


def solution(mesh):
    split = P(None, None, None, None, AXES)
    return jax.shard_map(
        per_device,
        mesh=mesh,
        in_specs=(P(None, AXES), P(AXES), P(), P(), split, split),
        out_specs=(split, split),
        check_vma=False,
    )
```
